128 devices in a mesh: tp: 64 (over z, y, x), dp: 2 (over core).
Axes of the slice: x: 4, y: 4, z: 4, core: 2. Of those that a mesh axis runs over, the one named last changes fastest.
Arguments:
- x_in: bfloat16 [128, 3072], P('dp')
- w_gate: bfloat16 [3072, 24576], P('dp', 'tp')
- w_up: bfloat16 [3072, 24576], P('dp', 'tp')
- w_down: bfloat16 [24576, 3072], P('tp', 'dp')
- dy_in: bfloat16 [128, 3072], P('dp')
Outputs:
- output 1: bfloat16 [128, 3072], P('dp')
- output 2: bfloat16 [128, 3072], P('dp')
- output 3: float32 [3072, 24576], P('dp', 'tp')
- output 4: float32 [3072, 24576], P('dp', 'tp')
- output 5: float32 [24576, 3072], P('tp', 'dp')
All inputs are finite; a program needn't handle non-finite values.
Results may differ from the reference program's by a relative error of at most 0.001.
Values are sent between devices in bfloat16 or wider.
A program may use at most 1 GiB of HBM per device.

```python
import jax
import jax.numpy as jnp
from jax import lax

MODEL_DIM = 3072
HIDDEN_DIM = 24576
SHARD_TOKENS = 64
DATA_SHARDS = 2


def setup_inputs(seed: int = 0) -> dict:
    key_list = jax.random.split(jax.random.key(seed), 5)
    row_count = DATA_SHARDS * SHARD_TOKENS
    x_vals = jax.random.normal(key_list[0], (row_count, MODEL_DIM), jnp.float32)
    gate_vals = jax.random.normal(key_list[1], (MODEL_DIM, HIDDEN_DIM), jnp.float32) * MODEL_DIM ** -0.5
    up_vals = jax.random.normal(key_list[2], (MODEL_DIM, HIDDEN_DIM), jnp.float32) * MODEL_DIM ** -0.5
    down_vals = jax.random.normal(key_list[3], (HIDDEN_DIM, MODEL_DIM), jnp.float32) * HIDDEN_DIM ** -0.5
    dy_vals = jax.random.normal(key_list[4], (row_count, MODEL_DIM), jnp.float32)
    return {
        'x_in': x_vals.astype(jnp.bfloat16),
        'w_gate': gate_vals.astype(jnp.bfloat16),
        'w_up': up_vals.astype(jnp.bfloat16),
        'w_down': down_vals.astype(jnp.bfloat16),
        'dy_in': dy_vals.astype(jnp.bfloat16),
    }


def reference(x_in, w_gate, w_up, w_down, dy_in):
    row_count = DATA_SHARDS * SHARD_TOKENS
    x_blocks = x_in.reshape(DATA_SHARDS, SHARD_TOKENS, MODEL_DIM)
    dy_blocks = dy_in.reshape(DATA_SHARDS, SHARD_TOKENS, MODEL_DIM)

    def shard_pass(carry, block):
        acc_gate, acc_up, acc_down = carry
        x_blk, dy_blk = block
        gate_pre = jnp.dot(x_blk, w_gate, preferred_element_type=jnp.float32)
        up_pre = jnp.dot(x_blk, w_up, preferred_element_type=jnp.float32)
        sig_gate = jax.nn.sigmoid(gate_pre)
        silu_gate = gate_pre * sig_gate
        hidden = (silu_gate * up_pre).astype(jnp.bfloat16)
        y_blk = (x_blk.astype(jnp.float32) + jnp.dot(hidden, w_down, preferred_element_type=jnp.float32)).astype(jnp.bfloat16)
        grad_h = jnp.dot(dy_blk, w_down.T, preferred_element_type=jnp.float32)
        d_gate = (grad_h * up_pre * sig_gate * (1.0 + gate_pre * (1.0 - sig_gate))).astype(jnp.bfloat16)
        d_up = (grad_h * silu_gate).astype(jnp.bfloat16)
        dx_blk = (dy_blk.astype(jnp.float32)
                  + jnp.dot(d_gate, w_gate.T, preferred_element_type=jnp.float32)
                  + jnp.dot(d_up, w_up.T, preferred_element_type=jnp.float32)).astype(jnp.bfloat16)
        acc_gate = acc_gate + jnp.dot(x_blk.T, d_gate, preferred_element_type=jnp.float32)
        acc_up = acc_up + jnp.dot(x_blk.T, d_up, preferred_element_type=jnp.float32)
        acc_down = acc_down + jnp.dot(hidden.T, dy_blk, preferred_element_type=jnp.float32)
        return (acc_gate, acc_up, acc_down), (y_blk, dx_blk)

    zero_acc = (jnp.zeros((MODEL_DIM, HIDDEN_DIM), jnp.float32),
                jnp.zeros((MODEL_DIM, HIDDEN_DIM), jnp.float32),
                jnp.zeros((HIDDEN_DIM, MODEL_DIM), jnp.float32))
    sums, outs = lax.scan(shard_pass, zero_acc, (x_blocks, dy_blocks))
    y_blocks, dx_blocks = outs
    return (y_blocks.reshape(row_count, MODEL_DIM), dx_blocks.reshape(row_count, MODEL_DIM), sums[0], sums[1], sums[2])
```

```python
import functools

import jax
import jax.numpy as jnp
from jax import lax
from jax.experimental import pallas as pl
from jax.experimental.pallas import tpu as pltpu
from jax.sharding import PartitionSpec as P

F32, BF16 = jnp.float32, jnp.bfloat16
ROWS, WIDTH, HALF, HID = 64, 3072, 1536, 384
PLANE = [(o2, o3) for o3 in range(4) for o2 in range(4) if o2 or o3]


def nt_dot(lhs, rhs):
    return lax.dot_general(lhs, rhs, (((1,), (1,)), ((), ())), preferred_element_type=F32)


def tn_dot(lhs, rhs):
    return lax.dot_general(lhs, rhs, (((0,), (0,)), ((), ())), preferred_element_type=F32)


def layer_kernel(x_hbm, wg_hbm, wu_hbm, wd_hbm, dy_hbm,
                 xc, dyc, hid, dga, dup, gath,
                 xv, dyv, wg, wu, wd, part, rpart, psum, recv1, mid, recv2, tiles15,
                 ld, xs, xr, ps, pr, s1s, s1r, s2s, s2r, s3s, s3r, s4s, s4r):
    t, c = lax.axis_index("tp"), lax.axis_index("dp")
    pos = [lax.rem(t, 4), lax.rem(t // 4, 4), t // 16]
    step = [1, 4, 16]
    delta = [[0 if o == 0 else (lax.rem(pos[d] + o, 4) - pos[d]) * step[d] for o in range(4)] for d in range(3)]

    def remote(src, dst, send, recv, tp, core):
        pltpu.make_async_remote_copy(src_ref=src, dst_ref=dst, send_sem=send, recv_sem=recv,
                                     device_id=(tp, core), device_id_type=pl.DeviceIdType.MESH).start()

    def wait_bytes(ref, sem):
        pltpu.make_async_copy(ref, ref, sem).wait()

    mine = pl.ds(pl.multiple_of(c * HALF, HALF), HALF)
    other = pl.ds(pl.multiple_of((1 - c) * HALF, HALF), HALF)
    own_rows, peer_rows = pl.ds(0, ROWS), pl.ds(ROWS, ROWS)
    loads = [pltpu.make_async_copy(x_hbm, xv, ld.at[0]),
             pltpu.make_async_copy(dy_hbm, dyv, ld.at[1]),
             pltpu.make_async_copy(x_hbm.at[:, mine], xc.at[own_rows], ld.at[2]),
             pltpu.make_async_copy(wg_hbm, wg, ld.at[3]),
             pltpu.make_async_copy(wu_hbm, wu, ld.at[4]),
             pltpu.make_async_copy(dy_hbm.at[:, mine], dyc.at[own_rows], ld.at[5]),
             pltpu.make_async_copy(wd_hbm, wd, ld.at[6])]
    barrier = pltpu.get_barrier_semaphore()
    pl.semaphore_signal(barrier, 1, device_id=(t, 1 - c), device_id_type=pl.DeviceIdType.MESH)
    for d in range(3):
        for o in range(1, 4):
            pl.semaphore_signal(barrier, 1, device_id=(t + delta[d][o], c), device_id_type=pl.DeviceIdType.MESH)
    for cp in loads:
        cp.start()
    loads[0].wait()
    loads[1].wait()
    pl.semaphore_wait(barrier, 10)

    remote(xv.at[:, other], xc.at[peer_rows], xs.at[0], xr.at[0], t, 1 - c)
    remote(dyv.at[:, other], dyc.at[peer_rows], xs.at[1], xr.at[1], t, 1 - c)

    def send_part(m, val):
        part[m, 1] = val[:ROWS]
        part[m, 0] = val[ROWS:]
        remote(part.at[m], rpart.at[m], ps.at[m], pr.at[m], t, 1 - c)

    loads[2].wait()
    loads[3].wait()
    wait_bytes(xc.at[peer_rows], xr.at[0])
    send_part(0, jnp.dot(xc[...], wg[...], preferred_element_type=F32))
    loads[4].wait()
    send_part(1, jnp.dot(xc[...], wu[...], preferred_element_type=F32))
    loads[5].wait()
    loads[6].wait()
    wait_bytes(dyc.at[peer_rows], xr.at[1])
    send_part(2, nt_dot(dyc[...], wd[...]))

    def full(m, e):
        return part[m, 1 - e] + rpart[m, e]

    def send1(j, a):
        for o in range(4):
            for e in range(2):
                if o or e:
                    slot = (o - 1) * 2 + e if o else 6
                    k = lax.rem(pos[j] + o, 4)
                    remote(psum.at[j, k, e, a], recv1.at[j, slot, a], s1s, s1r.at[j], t + delta[j][o],
                           1 - c if e else c)

    def put(j, a, val):
        for e in range(2):
            for r in range(4):
                for q in range(4):
                    psum[j, r, e, a, q] = val[e * 64 + r * 16:e * 64 + r * 16 + 16, q * 128:q * 128 + 128]

    wait_bytes(rpart.at[0], pr.at[0])
    wait_bytes(rpart.at[1], pr.at[1])
    for e in range(2):
        gate = full(0, e)
        hid[e * ROWS:(e + 1) * ROWS, :] = (gate * jax.nn.sigmoid(gate) * full(1, e)).astype(BF16)
    for j in range(3):
        put(j, 0, jnp.dot(hid[...], wd[:, j * 512:(j + 1) * 512], preferred_element_type=F32))
        send1(j, 0)
    wait_bytes(rpart.at[2], pr.at[2])
    for e in range(2):
        gate, up, grad = full(0, e), full(1, e), full(2, e)
        sig = jax.nn.sigmoid(gate)
        rows = slice(e * ROWS, (e + 1) * ROWS)
        dga[rows, :] = (grad * up * sig * (1.0 + gate * (1.0 - sig))).astype(BF16)
        dup[rows, :] = (grad * (gate * sig)).astype(BF16)
    for j in range(3):
        cols = slice(j * 512, (j + 1) * 512)
        put(j, 1, nt_dot(dga[...], wg[cols, :]) + nt_dot(dup[...], wu[cols, :]))
        send1(j, 1)

    def sum1_send2(j):
        d2, d3 = (j + 1) % 3, (j + 2) % 3
        mid[j, 0] = psum[j, pos[j], 0] + recv1[j, 0] + recv1[j, 2] + recv1[j, 4]
        mid[j, 1] = recv1[j, 6] + recv1[j, 1] + recv1[j, 3] + recv1[j, 5]
        for n, (o2, o3) in enumerate(PLANE):
            i2, i3 = lax.rem(pos[d2] + o2, 4), lax.rem(pos[d3] + o3, 4)
            remote(mid.at[j, lax.rem(i3 // 2 + c, 2), lax.rem(i3, 2), i2], recv2.at[j, n], s2s, s2r.at[j],
                   t + delta[d2][o2] + delta[d3][o3], c)

    wait_bytes(recv1.at[0], s1r.at[0])
    wait_bytes(recv1.at[1], s1r.at[1])
    sum1_send2(0)
    sum1_send2(1)
    wait_bytes(recv1.at[2], s1r.at[2])
    sum1_send2(2)

    for j in range(3):
        d2, d3 = (j + 1) % 3, (j + 2) % 3
        i1, i2, i3 = pos[j], pos[d2], pos[d3]
        half, which = i3 // 2, lax.rem(i3, 2)
        rows = pl.ds(pl.multiple_of(i1 * 16, 16), 16)
        cols = pl.ds(pl.multiple_of(half * HALF + j * 512 + i2 * 128, 128), 128)
        base = jnp.where(which == 0, xv[rows, cols].astype(F32), dyv[rows, cols].astype(F32))
        wait_bytes(recv2.at[j], s2r.at[j])
        total = mid[j, lax.rem(half + c, 2), which, i2]
        for n in range(15):
            total += recv2[j, n]
        gath[j, i1, i3, i2] = (base + total).astype(BF16)
        for o2, o3 in PLANE:
            remote(gath.at[j, i1, i3, i2], gath.at[j, i1, i3, i2], s3s.at[j], s3r.at[j],
                   t + delta[d2][o2] + delta[d3][o3], c)
    for j in range(3):
        wait_bytes(tiles15, s3r.at[j])
        for o in range(1, 4):
            remote(gath.at[j, pos[j]], gath.at[j, pos[j]], s4s, s4r.at[j], t + delta[j][o], c)
    wait_bytes(xv.at[:, other], xs.at[0])
    wait_bytes(dyv.at[:, other], xs.at[1])
    for m in range(3):
        wait_bytes(part.at[m], ps.at[m])
        wait_bytes(tiles15, s3s.at[m])
    wait_bytes(recv1, s1s)
    wait_bytes(recv2, s2s)
    for j in range(3):
        wait_bytes(gath.at[j, 0:3], s4r.at[j])
    wait_bytes(gath.at[:, 0:3], s4s)


def grad_kernel(xc, dyc, hid, dga, dup, gath, y_out, dx_out, dwg, dwu, dwd):
    i = pl.program_id(0)
    half, j = i // 3, lax.rem(i, 3)
    for a, out in enumerate((y_out, dx_out)):
        for r in range(4):
            for q in range(4):
                out[r * 16:(r + 1) * 16, q * 128:(q + 1) * 128] = gath[j, r, half * 2 + a, q]
    cols = pl.ds(pl.multiple_of(i * 256, 256), 256)
    xt = xc[:, cols]
    dwg[...] = tn_dot(xt, dga[...])
    dwu[...] = tn_dot(xt, dup[...])
    dwd[...] = tn_dot(hid[...], dyc[:, cols])


def solution(mesh):
    vmem = pl.BlockSpec(memory_space=pltpu.VMEM)
    hbm = pl.BlockSpec(memory_space=pl.ANY)
    sds = jax.ShapeDtypeStruct

    def device_pass(x_rows, gate_blk, up_blk, down_blk, dy_rows):
        mids = pl.pallas_call(
            layer_kernel,
            name="layer",
            out_shape=[sds((128, HALF), BF16), sds((128, HALF), BF16), sds((128, HID), BF16), sds((128, HID), BF16),
                       sds((128, HID), BF16), sds((3, 4, 4, 4, 16, 128), BF16)],
            in_specs=[hbm] * 5,
            out_specs=[vmem] * 6,
            scratch_shapes=[
                pltpu.VMEM((ROWS, WIDTH), BF16), pltpu.VMEM((ROWS, WIDTH), BF16),
                pltpu.VMEM((HALF, HID), BF16), pltpu.VMEM((HALF, HID), BF16), pltpu.VMEM((HID, HALF), BF16),
                pltpu.VMEM((3, 2, ROWS, HID), F32), pltpu.VMEM((3, 2, ROWS, HID), F32),
                pltpu.VMEM((3, 4, 2, 2, 4, 16, 128), F32), pltpu.VMEM((3, 7, 2, 4, 16, 128), F32),
                pltpu.VMEM((3, 2, 2, 4, 16, 128), F32), pltpu.VMEM((3, 15, 16, 128), F32),
                pltpu.VMEM((15, 16, 128), BF16),
                pltpu.SemaphoreType.DMA((7,)), pltpu.SemaphoreType.DMA((2,)), pltpu.SemaphoreType.DMA((2,)),
                pltpu.SemaphoreType.DMA((3,)), pltpu.SemaphoreType.DMA((3,)),
                pltpu.SemaphoreType.DMA, pltpu.SemaphoreType.DMA((3,)),
                pltpu.SemaphoreType.DMA, pltpu.SemaphoreType.DMA((3,)),
                pltpu.SemaphoreType.DMA((3,)), pltpu.SemaphoreType.DMA((3,)),
                pltpu.SemaphoreType.DMA, pltpu.SemaphoreType.DMA((3,)),
            ],
            compiler_params=pltpu.CompilerParams(collective_id=0, has_side_effects=True),
        )(x_rows, gate_blk, up_blk, down_blk, dy_rows)
        return tuple(pl.pallas_call(
            grad_kernel,
            name="grads",
            grid=(6,),
            out_shape=[sds((ROWS, WIDTH), BF16), sds((ROWS, WIDTH), BF16), sds((HALF, HID), F32), sds((HALF, HID), F32),
                       sds((HID, HALF), F32)],
            in_specs=[vmem] * 6,
            out_specs=[pl.BlockSpec((ROWS, 512), lambda i: (0, i)), pl.BlockSpec((ROWS, 512), lambda i: (0, i)),
                       pl.BlockSpec((256, HID), lambda i: (i, 0)), pl.BlockSpec((256, HID), lambda i: (i, 0)),
                       pl.BlockSpec((HID, 256), lambda i: (0, i))],
        )(*mids))

    row_spec = P('dp', None)
    weight_spec = P('dp', 'tp')
    down_spec = P('tp', 'dp')
    return jax.shard_map(device_pass, mesh=mesh,
                         in_specs=(row_spec, weight_spec, weight_spec, down_spec, row_spec),
                         out_specs=(row_spec, row_spec, weight_spec, weight_spec, down_spec),
                         check_vma=False)
```

```python
import jax
import jax.numpy as jnp
from jax import lax
from jax.experimental import pallas as pl
from jax.experimental.pallas import tpu as pltpu
from jax.sharding import PartitionSpec as P

F32, BF16 = jnp.float32, jnp.bfloat16
ROWS, WIDTH, HALF, HID = 64, 3072, 1536, 384
PLANE = [(o2, o3) for o3 in range(4) for o2 in range(4) if o2 or o3]


def nt_dot(lhs, rhs):
    return lax.dot_general(lhs, rhs, (((1,), (1,)), ((), ())), preferred_element_type=F32)


def tn_dot(lhs, rhs):
    return lax.dot_general(lhs, rhs, (((0,), (0,)), ((), ())), preferred_element_type=F32)


def layer_kernel(x_hbm, wg_hbm, wu_hbm, wd_hbm, dy_hbm,
                 dwg, dwu, dwd, gath,
                 xc, dyc, hid, dga, dup, xv, dyv, wg, wu, wd, part, rpart, psum, recv1, mid, recv2, tiles,
                 ld, xs, xr, ps, pr, s1s, s1r, s2s, s2r, s3s, s3r, s4s, s4r):
    t, c = lax.axis_index("tp"), lax.axis_index("dp")
    pos = [lax.rem(t, 4), lax.rem(t // 4, 4), t // 16]
    step = [1, 4, 16]
    delta = [[0 if o == 0 else (lax.rem(pos[d] + o, 4) - pos[d]) * step[d] for o in range(4)] for d in range(3)]

    def remote(src, dst, send, recv, tp, core):
        pltpu.make_async_remote_copy(src_ref=src, dst_ref=dst, send_sem=send, recv_sem=recv,
                                     device_id=(tp, core), device_id_type=pl.DeviceIdType.MESH).start()

    def wait_bytes(ref, sem):
        pltpu.make_async_copy(ref, ref, sem).wait()

    mine = pl.ds(pl.multiple_of(c * HALF, HALF), HALF)
    other = pl.ds(pl.multiple_of((1 - c) * HALF, HALF), HALF)
    own_rows, peer_rows = pl.ds(0, ROWS), pl.ds(ROWS, ROWS)
    loads = [pltpu.make_async_copy(x_hbm, xv, ld.at[0]),
             pltpu.make_async_copy(dy_hbm, dyv, ld.at[1]),
             pltpu.make_async_copy(x_hbm.at[:, mine], xc.at[own_rows], ld.at[2]),
             pltpu.make_async_copy(wg_hbm, wg, ld.at[3]),
             pltpu.make_async_copy(wu_hbm, wu, ld.at[4]),
             pltpu.make_async_copy(dy_hbm.at[:, mine], dyc.at[own_rows], ld.at[5]),
             pltpu.make_async_copy(wd_hbm, wd, ld.at[6])]
    barrier = pltpu.get_barrier_semaphore()
    pl.semaphore_signal(barrier, 1, device_id=(t, 1 - c), device_id_type=pl.DeviceIdType.MESH)
    for d in range(3):
        for o in range(1, 4):
            pl.semaphore_signal(barrier, 1, device_id=(t + delta[d][o], c), device_id_type=pl.DeviceIdType.MESH)
    for cp in loads:
        cp.start()
    loads[0].wait()
    loads[1].wait()
    pl.semaphore_wait(barrier, 10)

    remote(xv.at[:, other], xc.at[peer_rows], xs.at[0], xr.at[0], t, 1 - c)
    remote(dyv.at[:, other], dyc.at[peer_rows], xs.at[1], xr.at[1], t, 1 - c)

    def send_part(m, val):
        part[m, 1] = val[:ROWS]
        part[m, 0] = val[ROWS:]
        remote(part.at[m], rpart.at[m], ps.at[m], pr.at[m], t, 1 - c)

    loads[2].wait()
    loads[3].wait()
    wait_bytes(xc.at[peer_rows], xr.at[0])
    send_part(0, jnp.dot(xc[...], wg[...], preferred_element_type=F32))
    loads[4].wait()
    send_part(1, jnp.dot(xc[...], wu[...], preferred_element_type=F32))
    loads[5].wait()
    loads[6].wait()
    wait_bytes(dyc.at[peer_rows], xr.at[1])
    send_part(2, nt_dot(dyc[...], wd[...]))

    def full(m, e):
        return part[m, 1 - e] + rpart[m, e]

    def send1(j, a):
        for o in range(4):
            for e in range(2):
                if o or e:
                    slot = (o - 1) * 2 + e if o else 6
                    k = lax.rem(pos[j] + o, 4)
                    remote(psum.at[j, k, e, a], recv1.at[j, a, slot], s1s, s1r.at[j, a], t + delta[j][o],
                           1 - c if e else c)

    def put(j, a, val):
        for e in range(2):
            for r in range(4):
                for q in range(4):
                    psum[j, r, e, a, q] = val[e * 64 + r * 16:e * 64 + r * 16 + 16, q * 128:q * 128 + 128]

    wait_bytes(rpart.at[0], pr.at[0])
    wait_bytes(rpart.at[1], pr.at[1])
    for e in range(2):
        gate = full(0, e)
        hid[e * ROWS:(e + 1) * ROWS, :] = (gate * jax.nn.sigmoid(gate) * full(1, e)).astype(BF16)
    for j in range(3):
        put(j, 0, jnp.dot(hid[...], wd[:, j * 512:(j + 1) * 512], preferred_element_type=F32))
        send1(j, 0)
    wait_bytes(rpart.at[2], pr.at[2])
    for e in range(2):
        gate, up, grad = full(0, e), full(1, e), full(2, e)
        sig = jax.nn.sigmoid(gate)
        rows = slice(e * ROWS, (e + 1) * ROWS)
        dga[rows, :] = (grad * up * sig * (1.0 + gate * (1.0 - sig))).astype(BF16)
        dup[rows, :] = (grad * (gate * sig)).astype(BF16)
    for j in range(3):
        cols = slice(j * 512, (j + 1) * 512)
        put(j, 1, nt_dot(dga[...], wg[cols, :]) + nt_dot(dup[...], wu[cols, :]))
        send1(j, 1)
    for i in range(6):
        cols = slice(i * 256, (i + 1) * 256)
        dwd[:, cols] = tn_dot(hid[...], dyc[:, cols])
    for i in range(6):
        cols = slice(i * 256, (i + 1) * 256)
        dwg[cols, :] = tn_dot(xc[:, cols], dga[...])
        dwu[cols, :] = tn_dot(xc[:, cols], dup[...])

    def stage2(j, a):
        d2, d3 = (j + 1) % 3, (j + 2) % 3
        for e in range(2):
            own = recv1[j, a, 6] if e else psum[j, pos[j], 0, a]
            mid[j, a, e] = own + recv1[j, a, e] + recv1[j, a, 2 + e] + recv1[j, a, 4 + e]
        odd = lax.rem(pos[d3] + a, 2)
        for h in range(2):
            o3 = odd + 2 * h
            i3 = lax.rem(pos[d3] + o3, 4)
            for o2 in range(4):
                def send():
                    remote(mid.at[j, a, lax.rem(i3 // 2 + c, 2), lax.rem(pos[d2] + o2, 4)],
                           recv2.at[j, o3 * 4 + o2 - 1], s2s, s2r.at[j],
                           t + delta[d2][o2] + (i3 - pos[d3]) * step[d3], c)
                if h or o2:
                    send()
                else:
                    pl.when(odd == 1)(send)

    for a in range(2):
        wait_bytes(recv1.at[0, a], s1r.at[0, a])
        wait_bytes(recv1.at[1, a], s1r.at[1, a])
        stage2(0, a)
        stage2(1, a)
        wait_bytes(recv1.at[2, a], s1r.at[2, a])
        stage2(2, a)

    def stage3(j, a):
        d2, d3 = (j + 1) % 3, (j + 2) % 3
        i1, i2, half = pos[j], pos[d2], pos[d3] // 2
        rows = pl.ds(pl.multiple_of(i1 * 16, 16), 16)
        cols = pl.ds(pl.multiple_of(half * HALF + j * 512 + i2 * 128, 128), 128)
        base = (dyv if a else xv)[rows, cols].astype(F32)
        wait_bytes(recv2.at[j], s2r.at[j])
        total = mid[j, a, lax.rem(half + c, 2), i2]
        for n in range(15):
            total += recv2[j, n]
        gath[j, i1, a, half, i2] = (base + total).astype(BF16)
        for o2, o3 in PLANE:
            remote(gath.at[j, i1, a, half, i2], gath.at[j, i1, a, half, i2], s3s.at[j], s3r.at[j, a],
                   t + delta[d2][o2] + delta[d3][o3], c)

    for a in range(2):
        for j in range(3):
            pl.when(lax.rem(pos[(j + 2) % 3], 2) == a)(lambda: stage3(j, a))
    for a in range(2):
        for j in range(3):
            owner = lax.rem(pos[(j + 2) % 3], 2) == a
            pl.when(owner)(lambda: wait_bytes(tiles.at[0:7], s3r.at[j, a]))
            pl.when(jnp.logical_not(owner))(lambda: wait_bytes(tiles.at[0:8], s3r.at[j, a]))
            for o in range(1, 4):
                remote(gath.at[j, pos[j], a], gath.at[j, pos[j], a], s4s, s4r.at[j, a], t + delta[j][o], c)
    wait_bytes(xv.at[:, other], xs.at[0])
    wait_bytes(dyv.at[:, other], xs.at[1])
    for m in range(3):
        wait_bytes(part.at[m], ps.at[m])
        wait_bytes(tiles, s3s.at[m])
    wait_bytes(recv1, s1s)
    wait_bytes(recv2, s2s)
    for a in range(2):
        for j in range(3):
            wait_bytes(gath.at[j, 0:3, a], s4r.at[j, a])
    wait_bytes(gath.at[:, 0:3], s4s)


def flush_kernel(dwg, dwu, dwd, gath, y_out, dx_out, dwg_out, dwu_out, dwd_out, rows, sem):
    copies = []
    for n, (src, dst) in enumerate(((dwg, dwg_out), (dwu, dwu_out), (dwd, dwd_out))):
        size = src.shape[0] // 4
        for k in range(4):
            part = pl.ds(k * size, size)
            copies.append(pltpu.make_async_copy(src.at[part], dst.at[part], sem.at[4 * n + k]))
            copies[-1].start()
    for a, out in enumerate((y_out, dx_out)):
        for j in range(3):
            for half in range(2):
                for r in range(4):
                    for q in range(4):
                        col = half * HALF + j * 512 + q * 128
                        rows[a, r * 16:(r + 1) * 16, col:col + 128] = gath[j, r, a, half, q]
        copies.append(pltpu.make_async_copy(rows.at[a], out, sem.at[12 + a]))
        copies[-1].start()
    for cp in copies:
        cp.wait()


def solution(mesh):
    vmem = pl.BlockSpec(memory_space=pltpu.VMEM)
    hbm = pl.BlockSpec(memory_space=pltpu.HBM)
    sds = jax.ShapeDtypeStruct

    def device_pass(x_rows, gate_blk, up_blk, down_blk, dy_rows):
        results = pl.pallas_call(
            layer_kernel,
            name="layer",
            out_shape=[pltpu.VMEM((HALF, HID), F32), pltpu.VMEM((HALF, HID), F32), pltpu.VMEM((HID, HALF), F32),
                       pltpu.VMEM((3, 4, 2, 2, 4, 16, 128), BF16)],
            in_specs=[hbm] * 5,
            out_specs=[vmem] * 4,
            scratch_shapes=[
                pltpu.VMEM((128, HALF), BF16), pltpu.VMEM((128, HALF), BF16),
                pltpu.VMEM((128, HID), BF16), pltpu.VMEM((128, HID), BF16), pltpu.VMEM((128, HID), BF16),
                pltpu.VMEM((ROWS, WIDTH), BF16), pltpu.VMEM((ROWS, WIDTH), BF16),
                pltpu.VMEM((HALF, HID), BF16), pltpu.VMEM((HALF, HID), BF16), pltpu.VMEM((HID, HALF), BF16),
                pltpu.VMEM((3, 2, ROWS, HID), F32), pltpu.VMEM((3, 2, ROWS, HID), F32),
                pltpu.VMEM((3, 4, 2, 2, 4, 16, 128), F32), pltpu.VMEM((3, 2, 7, 4, 16, 128), F32),
                pltpu.VMEM((3, 2, 2, 4, 16, 128), F32), pltpu.VMEM((3, 15, 16, 128), F32),
                pltpu.VMEM((15, 16, 128), BF16),
                pltpu.SemaphoreType.DMA((7,)), pltpu.SemaphoreType.DMA((2,)), pltpu.SemaphoreType.DMA((2,)),
                pltpu.SemaphoreType.DMA((3,)), pltpu.SemaphoreType.DMA((3,)),
                pltpu.SemaphoreType.DMA, pltpu.SemaphoreType.DMA((3, 2)),
                pltpu.SemaphoreType.DMA, pltpu.SemaphoreType.DMA((3,)),
                pltpu.SemaphoreType.DMA((3,)), pltpu.SemaphoreType.DMA((3, 2)),
                pltpu.SemaphoreType.DMA, pltpu.SemaphoreType.DMA((3, 2)),
            ],
            compiler_params=pltpu.CompilerParams(collective_id=0, has_side_effects=True, vmem_limit_bytes=59000000),
        )(x_rows, gate_blk, up_blk, down_blk, dy_rows)
        return tuple(pl.pallas_call(
            flush_kernel,
            name="flush",
            out_shape=[sds((ROWS, WIDTH), BF16), sds((ROWS, WIDTH), BF16), sds((HALF, HID), F32), sds((HALF, HID), F32),
                       sds((HID, HALF), F32)],
            in_specs=[vmem] * 4,
            out_specs=[hbm] * 5,
            scratch_shapes=[pltpu.VMEM((2, ROWS, WIDTH), BF16), pltpu.SemaphoreType.DMA((14,))],
            compiler_params=pltpu.CompilerParams(vmem_limit_bytes=16 * 2**20),
        )(*results))

    row_spec = P('dp', None)
    weight_spec = P('dp', 'tp')
    down_spec = P('tp', 'dp')
    return jax.shard_map(device_pass, mesh=mesh,
                         in_specs=(row_spec, weight_spec, weight_spec, down_spec, row_spec),
                         out_specs=(row_spec, row_spec, weight_spec, weight_spec, down_spec),
                         check_vma=False)
```
